256 devices in a mesh: expert: 128 (over y_lo, z, x, core), dp: 2 (over y_hi).
Axes of the slice: x: 4, y: 4 (y_hi: 2, y_lo: 2; y = y_hi * 2 + y_lo), z: 8, core: 2. Of those that a mesh axis runs over, the one named last changes fastest.
Arguments:
- tokens: bfloat16 [32768, 2560], P(('expert', 'dp')), may hold values from -6 to 6
- routes: int32 [32768, 6], P(('expert', 'dp')), may hold values from 0 to 31, all different within a row; in each aligned block of 128 rows (0 to 127, 128 to 255, ...) at most 32 rows name the same one
- combine_weight: float32 [32768, 6], P(('expert', 'dp')), may hold values from 0.05 to 1
- owner_plan: int32 [32], replicated, may hold values from 0 to 31, as said below
- w_in: bfloat16 [2, 24576, 2560], P(None, 'expert', 'dp'), may hold values from -0.125 to 0.125
- w_out: bfloat16 [24576, 2560], P('expert', 'dp'), may hold values from -0.21875 to 0.21875
- grad_in: bfloat16 [2, 2, 24576, 2560], P('dp', None, 'expert'), may hold values from -6 to 6
- grad_out: bfloat16 [2, 24576, 2560], P('dp', 'expert'), may hold values from -6 to 6
- first_in: bfloat16 [2, 24576, 2560], P(None, 'expert', 'dp'), may hold values from -3 to 3
- second_in: bfloat16 [2, 24576, 2560], P(None, 'expert', 'dp'), may hold values from 0.25 to 4
- first_out: bfloat16 [24576, 2560], P('expert', 'dp'), may hold values from -3 to 3
- second_out: bfloat16 [24576, 2560], P('expert', 'dp'), may hold values from 0.25 to 4
Outputs:
- combined: bfloat16 [32768, 2560], P(('expert', 'dp'))
- first_in_next: bfloat16 [2, 24576, 2560], P(None, 'expert', 'dp')
- second_in_next: bfloat16 [2, 24576, 2560], P(None, 'expert', 'dp')
- first_out_next: bfloat16 [24576, 2560], P('expert', 'dp')
- second_out_next: bfloat16 [24576, 2560], P('expert', 'dp')
The draws below stay inside these ranges and needn't reach their ends.
Inputs may be any that keep to these rules, and one draw needn't show every extreme that they name: owner_plan is an involution: exactly 4 pairs of experts trade owners, every other expert maps to itself. `routes`: in the rows of one device (128 rows) no expert is named by more than 32 rows, a bound that some expert reaches in some device.
All inputs are finite; a program needn't handle non-finite values.
Results may differ from the reference program's by a relative error of at most 0.014.
Values may be sent and summed in bfloat16 or wider, within the bound.
A program may use at most 192 MiB of HBM per device.

```python
import math
import jax
import jax.numpy as jnp
import numpy as np
from jax import lax

D = 2560
HID = 768
GROUP = 4
TOK_DEV = 128
HDEV = 192
EXPERTS = 32
TOP = 6
MOVED = 4
CAP = 32
TOKENS = 32768
N_DP = 2
DEVICES = 256


def draw_owner_plan(key, part):
    shuffled = jax.random.permutation(jax.random.fold_in(key, 7), EXPERTS).astype(jnp.int32)
    expert_ids = jnp.arange(EXPERTS, dtype=jnp.int32)
    leaving = shuffled[:MOVED]
    arriving = shuffled[MOVED:2 * MOVED]
    owner_plan = expert_ids.at[leaving].set(arriving).at[arriving].set(leaving)
    return owner_plan.astype(jnp.int32)


def shard_levels(stream_key, dims, cuts, low, top_value):
    factor_of = 1.0
    for axis_at, parts in cuts:
        heights = jax.random.uniform(jax.random.fold_in(jax.random.fold_in(stream_key, 6), axis_at), (parts,), jnp.float32, low / len(cuts), top_value / len(cuts))
        factor_of = factor_of * jnp.repeat(jnp.exp(heights), dims[axis_at] // parts).reshape((-1,) + (1,) * (len(dims) - 1 - axis_at))
    return factor_of


def deal_out(key, own, number, rows, number_of, top, bound, slope):
    order = jax.random.permutation(key, number_of)
    packed, common = portions_of(number_of, rows * top, bound, slope, True), portions_of(number_of, rows * top, bound, slope, False)
    places = jnp.arange(number_of)

    def named(lengths, offset_by):
        used = int((lengths > 0).sum())
        fixed = max(1, used // 4)
        moved = fixed + (places - fixed + offset_by * (used - fixed)) % max(1, number_of - fixed)
        return jnp.zeros((number_of,), jnp.int32).at[order[jnp.where(places < fixed, places, moved)]].set(jnp.asarray(lengths, jnp.int32))

    lengths = jnp.where(number % 4 == 0, named(packed, number // 4), named(common, number - number // 4 - 1))
    mixed = jax.random.permutation(jax.random.fold_in(own, 3), number_of)
    giver, taker = mixed[0:number_of // 2 * 2:2], mixed[1:number_of // 2 * 2:2]
    slack = jnp.minimum(lengths[giver] - 1, bound - lengths[taker]) // 2
    slack = jnp.where((giver == order[0]) | (taker == order[0]) | (lengths[taker] == 0), 0, jnp.maximum(slack, 0))
    moved = jax.random.randint(jax.random.fold_in(own, 4), (number_of // 2,), 0, 1 << 20) % (slack + 1)
    lengths = lengths.at[giver].add(-moved).at[taker].add(moved)
    members = jnp.searchsorted(jnp.cumsum(lengths), jnp.arange(rows * top), side="right").astype(jnp.int32)
    listing = members.reshape(top, rows).T
    listing = listing[jax.random.permutation(jax.random.fold_in(own, 1), rows)]
    offset_by = jax.random.randint(jax.random.fold_in(own, 2), (rows, 1), 0, top)
    return jnp.take_along_axis(listing, (jnp.arange(top)[None, :] + offset_by) % top, axis=1)


def portions_of(amount, total, bound, slope, full):
    loads = [(1 << 20) // math.isqrt(rank ** slope) + 1 for rank in range(1, amount + 1)]
    largest = bound if full else min(bound, max(-(-total // amount), total * loads[0] // sum(loads)))
    least = 1 if total - largest >= amount - 1 else 0
    counts, rest = [largest] + [least] * (amount - 1), total - largest - least * (amount - 1)
    while rest > 0:
        candidates = [i for i in range(1, amount) if counts[i] < largest] or [i for i in range(1, amount) if counts[i] < bound]
        pool, left = sum([loads[i] for i in candidates]), rest
        for i in candidates:
            extra = min(bound - counts[i], max(1, left * loads[i] // pool), rest)
            counts[i] = counts[i] + extra
            rest = rest - extra
    return np.array(counts)


def noise(rng, extent, scale, limit, shards=(), held_as=jnp.bfloat16):
    array = jax.random.normal(rng, extent, jnp.float32) * scale
    if len(shards) > 0:
        array = shard_levels(rng, extent, shards, -0.22, 0.18) * array
    return jnp.clip(array, min=-limit, max=limit).astype(held_as)


def setup_inputs(seed: int = 0) -> dict:
    keys = jax.random.split(jax.random.key(seed), 13)
    tokens = noise(keys[0], (TOKENS, D), 1.0, 6.0, ((0, 256),))
    routes_keys = jax.random.split(jax.random.fold_in(keys[1], 1), TOKENS // TOK_DEV)
    routes_turns = jax.random.permutation(jax.random.fold_in(keys[1], 3), TOKENS // TOK_DEV)
    routes = jax.vmap(lambda own, number: deal_out(jax.random.fold_in(keys[1], 2), own, number, TOK_DEV, EXPERTS, TOP, CAP, 2))(routes_keys, routes_turns).reshape((TOKENS, TOP))
    combine_weight = jnp.clip(jnp.exp(math.log(1.0) - 2.9957323 * jax.random.uniform(keys[2], (TOKENS, TOP), jnp.float32) ** shard_levels(keys[2], (TOKENS, TOP), ((0, 256),), -0.2, 0.2)), 0.05, 1.0)
    owner_plan = draw_owner_plan(jax.random.fold_in(keys[12], 71), 0)
    w_in = noise(keys[4], (2, EXPERTS * HID, D), D ** -0.5, 0.125, ((1, 128), (2, 2)))
    w_out = noise(keys[5], (EXPERTS * HID, D), HID ** -0.5, 0.21875, ((0, 128), (1, 2)))
    grad_in = noise(keys[6], (N_DP, 2, EXPERTS * HID, D), 1.0, 6.0, ((0, 2), (2, 128)))
    grad_out = noise(keys[7], (N_DP, EXPERTS * HID, D), 1.0, 6.0, ((0, 2), (1, 128)))
    first_in = noise(keys[8], (2, EXPERTS * HID, D), 0.5, 3.0, ((1, 128), (2, 2)))
    second_in = jnp.clip(jnp.exp(math.log(4.0) - 2.7725887 * jax.random.uniform(keys[9], (2, EXPERTS * HID, D), jnp.float32) ** shard_levels(keys[9], (2, EXPERTS * HID, D), ((1, 128), (2, 2)), -0.2, 0.2)), 0.25, 4.0).astype(jnp.bfloat16)
    first_out = noise(keys[10], (EXPERTS * HID, D), 0.5, 3.0, ((0, 128), (1, 2)))
    second_out = jnp.clip(jnp.exp(math.log(4.0) - 2.7725887 * jax.random.uniform(keys[11], (EXPERTS * HID, D), jnp.float32) ** shard_levels(keys[11], (EXPERTS * HID, D), ((0, 128), (1, 2)), -0.2, 0.2)), 0.25, 4.0).astype(jnp.bfloat16)
    return dict(tokens=tokens, routes=routes, combine_weight=combine_weight, owner_plan=owner_plan, w_in=w_in, w_out=w_out, grad_in=grad_in, grad_out=grad_out, first_in=first_in, second_in=second_in, first_out=first_out, second_out=second_out)


BETA_ONE = 0.9
BETA_TWO = 0.95
LEARNING_RATE = 0.005
EPSILON = 1e-08
CORRECT_FIRST = 1.0 / (1.0 - 0.9 ** 10)
CORRECT_SECOND = 1.0 / (1.0 - 0.95 ** 10)

def adam_update(weight, gradient, first_moment, second_moment):
    first_next = BETA_ONE * first_moment.astype(jnp.float32) + (1.0 - BETA_ONE) * gradient
    second_next = BETA_TWO * second_moment.astype(jnp.float32) + (1.0 - BETA_TWO) * gradient * gradient
    stepped = weight.astype(jnp.float32) - LEARNING_RATE * (first_next * CORRECT_FIRST) / (jnp.sqrt(second_next * CORRECT_SECOND) + EPSILON)
    return (stepped.astype(jnp.bfloat16), first_next.astype(jnp.bfloat16), second_next.astype(jnp.bfloat16))

def slot_ranks(flat_routes):
    onehot = (flat_routes[:, None] == jnp.arange(EXPERTS, dtype=jnp.int32)[None, :]).astype(jnp.int32)
    ranks = jnp.cumsum(onehot, axis=0) - 1
    return lax.optimization_barrier(jnp.sum(ranks * onehot, axis=1)).astype(jnp.int32)

def times_rows(row_data, weight_rows):
    return lax.dot_general(row_data, weight_rows, (((1,), (1,)), ((), ())), preferred_element_type=jnp.float32)

def expert_rows(row_data, weight_in, weight_out):
    gate = times_rows(row_data, weight_in[0])
    upward = times_rows(row_data, weight_in[1])
    hidden = (jax.nn.silu(gate) * upward).astype(jnp.bfloat16)
    return jnp.dot(hidden, weight_out, preferred_element_type=jnp.float32).astype(jnp.bfloat16)

def expert_output(row_data, weight_in, weight_out):
    total = jnp.zeros((row_data.shape[0], weight_out.shape[1]), jnp.float32)
    for quarter in range(GROUP):
        begin = quarter * HDEV
        total = total + expert_rows(row_data, weight_in[:, begin:begin + HDEV], weight_out[begin:begin + HDEV]).astype(jnp.float32)
    return total.astype(jnp.bfloat16)

def reference(tokens, routes, combine_weight, owner_plan, w_in, w_out, grad_in, grad_out, first_in, second_in, first_out, second_out):
    width = tokens.shape[1]
    sum_in = lax.optimization_barrier(jnp.sum(grad_in.astype(jnp.float32), axis=0))
    sum_out = lax.optimization_barrier(jnp.sum(grad_out.astype(jnp.float32), axis=0))
    new_in, first_in_next, second_in_next = adam_update(w_in, sum_in, first_in, second_in)
    new_out, first_out_next, second_out_next = adam_update(w_out, sum_out, first_out, second_out)

    def regroup_in(moment):
        return jnp.take(moment.reshape(2, EXPERTS, HID, width), owner_plan, axis=1).reshape(moment.shape)

    def regroup_out(moment):
        return jnp.take(moment.reshape(EXPERTS, HID, width), owner_plan, axis=0).reshape(moment.shape)
    device_routes = routes.reshape(DEVICES, TOK_DEV * TOP)
    ranks = jax.vmap(slot_ranks)(device_routes)
    targets = (device_routes * CAP + ranks).astype(jnp.int32)
    token_ids = jnp.arange(TOKENS, dtype=jnp.int32).reshape(DEVICES, TOK_DEV)
    token_of_route = jnp.repeat(token_ids, TOP, axis=1)
    device_ids = jnp.repeat(jnp.arange(DEVICES, dtype=jnp.int32)[:, None], TOK_DEV * TOP, axis=1)
    table = jnp.zeros((DEVICES, EXPERTS * CAP), jnp.int32).at[device_ids, targets].set(token_of_route)
    weight_table = jnp.zeros((DEVICES, EXPERTS * CAP), jnp.float32).at[device_ids, targets].set(combine_weight.reshape(DEVICES, TOK_DEV * TOP))

    def one_expert(total, expert):
        start = (expert * CAP).astype(jnp.int32)
        row_ids = lax.dynamic_slice_in_dim(table, start, CAP, 1).reshape(-1)
        row_weights = lax.dynamic_slice_in_dim(weight_table, start, CAP, 1).reshape(-1)
        weight_in = lax.dynamic_slice_in_dim(new_in, (expert * HID).astype(jnp.int32), HID, 1)
        weight_out = lax.dynamic_slice_in_dim(new_out, (expert * HID).astype(jnp.int32), HID, 0)
        result = expert_output(tokens[row_ids], weight_in, weight_out)
        return (total.at[row_ids].add(row_weights[:, None] * result.astype(jnp.float32)), None)
    total, ignored = lax.scan(one_expert, jnp.zeros((TOKENS, width), jnp.float32), jnp.arange(EXPERTS, dtype=jnp.int32))
    return (total.astype(jnp.bfloat16), regroup_in(first_in_next), regroup_in(second_in_next), regroup_out(first_out_next), regroup_out(second_out_next))
```

```python
import functools
import jax
import jax.numpy as jnp
from jax import lax
from jax.experimental import pallas as pl
from jax.experimental.pallas import tpu as pltpu
from jax.sharding import Mesh, PartitionSpec as P

BETA_ONE = 0.9
BETA_TWO = 0.95
LEARNING_RATE = 0.005
EPSILON = 1e-08
CORRECT_FIRST = 1.0 / (1.0 - 0.9**10)
CORRECT_SECOND = 1.0 / (1.0 - 0.95**10)
CAP = 32
PLANE = 4
EXTRA = 128
EX = ("yl", "z", "xh", "xl", "c")
MESH = pl.DeviceIdType.MESH


def at_x(v):
    return {"xh": v // 2, "xl": v % 2}


def at_y(v):
    return {"dp": v // 2, "yl": v % 2}


def at_z(v):
    return {"z": v}


def place():
    x = lax.axis_index("xh") * 2 + lax.axis_index("xl")
    y = lax.axis_index("dp") * 2 + lax.axis_index("yl")
    return x, y, lax.axis_index("z"), lax.axis_index("c")


def greet(peers):
    barrier = pltpu.get_barrier_semaphore()
    for peer in peers:
        pl.semaphore_signal(barrier, inc=1, device_id=peer, device_id_type=MESH)
    pl.semaphore_wait(barrier, len(peers))


class Copies:
    def __init__(self, send_sems, recv_sems):
        self.send_sems, self.recv_sems, self.made = send_sems, recv_sems, []

    def send(self, src, dst, peer):
        i = len(self.made)
        copy = pltpu.make_async_remote_copy(
            src_ref=src,
            dst_ref=dst,
            send_sem=self.send_sems.at[i],
            recv_sem=self.recv_sems.at[i],
            device_id=peer,
            device_id_type=MESH,
        )
        copy.start()
        self.made.append(copy)
        return copy

    def finish(self):
        for copy in self.made:
            copy.wait_send()


N_GATHER = 40 + 8 + 9


def gather_kernel(tok_ref, w_ref, tok_out, w_out, send_sems, recv_sems, own_sems):
    x, y, z, c = place()
    xr, xl = (x + 1) % 4, (x + 3) % 4
    yr, yl = (y + 1) % 4, (y + 3) % 4
    zr, zl = (z + 1) % 8, (z + 7) % 8
    greet([at_x(xr), at_x(xl), at_y(yr), at_y(yl), at_z(zr), at_z(zl), {"c": 1 - c}])
    cs = Copies(send_sems, recv_sems)
    rows = w_ref.shape[1]
    h, q = rows // 2, rows // 4
    t = tok_ref.shape[0]

    def weights(slot, start, size):
        return w_out.at[slot, :, pl.ds(start, size)]

    def ring(base, slot_src, slot_of, peer_of, mine, src=None):
        right, left = (mine + 1) % 4, (mine + 3) % 4
        held = weights(slot_src, base, h) if src is None else src
        a = cs.send(held, weights(slot_src, base, h), peer_of(right))
        b = cs.send(held, weights(slot_src, base, h), peer_of(left))

        def forward():
            a.wait_recv()
            f = cs.send(
                weights(slot_of(left), base, q), weights(slot_of(left), base, q), peer_of(right)
            )
            b.wait_recv()
            g = cs.send(
                weights(slot_of(right), base + q, q),
                weights(slot_of(right), base + q, q),
                peer_of(left),
            )
            return f, g

        return forward

    def slot(yy, xx):
        return yy * 4 + xx

    own = slot(y, x)
    own_w = pltpu.make_async_copy(w_ref, w_out.at[own], own_sems.at[0])
    own_t = pltpu.make_async_copy(tok_ref, tok_out.at[z * 2 + c], own_sems.at[1])
    own_w.start()
    own_t.start()

    def x_ring(base, yy, src=None):
        return ring(base, slot(yy, x), lambda v: slot(yy, v), at_x, x, src)

    def y_ring(base, xx, src=None):
        return ring(base, slot(y, xx), lambda v: slot(v, xx), at_y, y, src)

    part_a, part_b = w_ref.at[:, pl.ds(0, h)], w_ref.at[:, pl.ds(h, h)]
    a1 = x_ring(0, y, part_a)
    b1 = y_ring(h, x, part_b)

    def tokens(place_z, half=None, core=c):
        ref = tok_out.at[place_z * 2 + core]
        return ref if half is None else ref.at[pl.ds(half * (t // 2), t // 2)]

    partner = {"c": 1 - c}
    t_r = cs.send(tok_ref, tokens(z), at_z(zr))
    t_l = cs.send(tok_ref, tokens(z), at_z(zl))
    kept = [cs.send(tok_ref, tokens(z), partner)]
    a2 = [y_ring(0, x, part_a)]
    b2 = [x_ring(h, y, part_b)]

    def token_step(s, last):
        nonlocal t_r, t_l
        from_l, from_r = (z + 8 - s) % 8, (z + s) % 8
        t_r.wait_recv()
        half = 0 if last else None
        n_r = cs.send(tokens(from_l, half), tokens(from_l, half), at_z(zr))
        t_l.wait_recv()
        half = 1 if last else None
        n_l = cs.send(tokens(from_r, half), tokens(from_r, half), at_z(zl))
        kept.append(cs.send(tokens(from_l), tokens(from_l), partner))
        kept.append(cs.send(tokens(from_r), tokens(from_r), partner))
        t_r, t_l = n_r, n_l

    f, g = a1()
    a2.append(y_ring(0, xl))
    a2.append(y_ring(0, xr))
    u, v = b1()
    b2.append(x_ring(h, yl))
    b2.append(x_ring(h, yr))
    token_step(1, False)
    f.wait_recv()
    g.wait_recv()
    a2.append(y_ring(0, (x + 2) % 4))
    u.wait_recv()
    v.wait_recv()
    b2.append(x_ring(h, (y + 2) % 4))
    ends = []
    ends += a2[0]()
    ends += b2[0]()
    token_step(2, False)
    ends += a2[1]()
    ends += b2[1]()
    token_step(3, True)
    ends += a2[2]()
    ends += b2[2]()
    t_r.wait_recv()
    t_l.wait_recv()
    far = (z + 4) % 8
    kept.append(cs.send(tokens(far, 0), tokens(far, 0), partner))
    kept.append(cs.send(tokens(far, 1), tokens(far, 1), partner))
    ends += a2[3]()
    ends += b2[3]()
    for copy in ends + kept:
        copy.wait_recv()
    cs.finish()
    own_w.wait()
    own_t.wait()


def gather_all(tok, w):
    sent = (w.size * 8 + tok.size * 4) * 2
    return pl.pallas_call(
        gather_kernel,
        out_shape=(
            jax.ShapeDtypeStruct((16, *tok.shape), tok.dtype),
            jax.ShapeDtypeStruct((16, *w.shape), w.dtype),
        ),
        in_specs=[pl.BlockSpec(memory_space=pltpu.HBM)] * 2,
        out_specs=(pl.BlockSpec(memory_space=pltpu.HBM),) * 2,
        scratch_shapes=[
            pltpu.SemaphoreType.DMA((N_GATHER + 2,)),
            pltpu.SemaphoreType.DMA((N_GATHER + 2,)),
            pltpu.SemaphoreType.DMA((2,)),
        ],
        compiler_params=pltpu.CompilerParams(collective_id=0, has_side_effects=True),
        cost_estimate=pl.CostEstimate(flops=0, bytes_accessed=400_000_000, transcendentals=0),
        name="gather_all",
    )(tok, w)


def moe_kernel(tok_ref, w_ref, out_ref, x_ref, slots_ref, weights_ref, *, width, top):
    j = pl.program_id(0)
    blocks, t = tok_ref.shape[0], tok_ref.shape[1]
    half = width // 2
    slots = PLANE * CAP

    @pl.when(j == 0)
    def _():
        z = lax.axis_index("z")
        lane = lax.broadcasted_iota(jnp.int32, (t, slots), 1)
        expert = (lane // (2 * CAP)) * 16 + z * 2 + (lane // CAP) % 2
        place_in = (expert * CAP + lane % CAP).astype(jnp.float32)

        def dispatch(b, _):
            info = tok_ref[b, :, width:].astype(jnp.float32)
            hit_any = jnp.zeros((t, slots), jnp.float32)
            total = jnp.zeros((t, slots), jnp.float32)
            for k in range(top):
                goal = info[:, k : k + 1] * CAP + info[:, top + k : top + k + 1]
                w = (
                    info[:, 2 * top + k : 2 * top + k + 1]
                    + info[:, 3 * top + k : 3 * top + k + 1]
                    + info[:, 4 * top + k : 4 * top + k + 1]
                )
                hit = goal == place_in
                hit_any = jnp.where(hit, 1.0, hit_any)
                total = jnp.where(hit, w, total)
            high = total.astype(jnp.bfloat16)
            low = (total - high.astype(jnp.float32)).astype(jnp.bfloat16)
            weights_ref[b] = jnp.concatenate([high, low], 1)
            rows = lax.dot_general(
                hit_any.astype(jnp.bfloat16),
                tok_ref[b, :, :width],
                (((0,), (0,)), ((), ())),
                preferred_element_type=jnp.float32,
            ).astype(jnp.bfloat16)
            for e in range(PLANE):
                x_ref[e, pl.ds(b * CAP, CAP), :] = rows[e * CAP : (e + 1) * CAP]
            return 0

        lax.fori_loop(0, blocks, dispatch, 0)

    dims = (((1,), (1,)), ((), ()))

    def chunk(m, _):
        mrows = 256
        at = pl.ds(m * mrows, mrows)
        x0, x1 = x_ref[j, at, :half], x_ref[j, at, half:]
        hidden = []
        for q in range(2):
            both = lax.dot_general(
                x0, w_ref[0, 0, 0, q, : 2 * 192], dims, preferred_element_type=jnp.float32
            ) + lax.dot_general(
                x1, w_ref[1, 0, 0, q, : 2 * 192], dims, preferred_element_type=jnp.float32
            )
            gate, up = both[:, :192], both[:, 192:]
            hidden.append((jax.nn.silu(gate) * up).astype(jnp.bfloat16))
        for d in range(2):
            out = jnp.dot(
                hidden[0], w_ref[d, 0, 0, 0, 2 * 192 :], preferred_element_type=jnp.float32
            ) + jnp.dot(
                hidden[1], w_ref[d, 0, 0, 1, 2 * 192 :], preferred_element_type=jnp.float32
            )
            x_ref[j, at, d * half : (d + 1) * half] = out.astype(jnp.bfloat16)
        return 0

    lax.fori_loop(0, blocks * CAP // 256, chunk, 0)

    @pl.when(j == PLANE - 1)
    def _():
        def combine(b, _):
            y = jnp.concatenate(
                [x_ref[e, pl.ds(b * CAP, CAP), :] for e in range(PLANE)], 0
            )
            y2 = jnp.concatenate([y, y], 0)
            out_ref[b] = jnp.dot(
                weights_ref[b], y2, preferred_element_type=jnp.float32
            ).astype(jnp.bfloat16)
            return 0

        lax.fori_loop(0, blocks, combine, 0)


def experts(all_tok, all_w, width, top):
    blocks, t, ext = all_tok.shape
    w = all_w.reshape(2, 2, 2, 2, 576, width // 2)
    whole = pl.BlockSpec(memory_space=pltpu.VMEM)
    return pl.pallas_call(
        functools.partial(moe_kernel, width=width, top=top),
        out_shape=jax.ShapeDtypeStruct((blocks, t, width), jnp.bfloat16),
        grid=(PLANE,),
        in_specs=[
            whole,
            pl.BlockSpec((2, 1, 1, 2, 576, width // 2), lambda j: (0, j // 2, j % 2, 0, 0, 0)),
        ],
        out_specs=whole,
        scratch_shapes=[
            pltpu.VMEM((PLANE, blocks * CAP, width), jnp.bfloat16),
            pltpu.VMEM((blocks, 8, 128), jnp.bfloat16),
            pltpu.VMEM((blocks, t, 2 * PLANE * CAP), jnp.bfloat16),
        ],
        compiler_params=pltpu.CompilerParams(vmem_limit_bytes=63 * 1024 * 1024),
        cost_estimate=pl.CostEstimate(
            flops=12_000_000_000, bytes_accessed=60_000_000, transcendentals=0
        ),
        name="experts",
    )(all_tok, w)


def add(a, b):
    return (a.astype(jnp.float32) + b.astype(jnp.float32)).astype(jnp.bfloat16)


N_SCATTER = 8 + 14


def scatter_kernel(p_ref, out_ref, cx, rr, rl, send_sems, recv_sems):
    x, y, z, c = place()
    zr, zl = (z + 1) % 8, (z + 7) % 8
    partner = {"c": 1 - c}
    greet([at_z(zr), at_z(zl), partner])
    cs = Copies(send_sems, recv_sems)
    t = out_ref.shape[0]
    h = t // 2
    order = [4, 3, 5, 2, 6, 1, 7, 0]
    swaps = {}
    for s in order:
        d = (z + s) % 8
        swaps[s] = cs.send(p_ref.at[d * 2 + (1 - c)], cx.at[s], partner)

    def own(s, rows):
        d = (z + s) % 8
        return add(p_ref[d * 2 + c, rows, :], cx[s, rows, :])

    low, high = pl.ds(0, h), pl.ds(h, h)
    swaps[4].wait_recv()
    cx[4, low, :] = own(4, low)
    far_r = cs.send(cx.at[4, low], rr.at[3, low], at_z(zr))
    cx[4, high, :] = own(4, high)
    far_l = cs.send(cx.at[4, high], rl.at[3, high], at_z(zl))
    swaps[3].wait_recv()
    swaps[5].wait_recv()
    cx[3, high, :] = own(3, high)
    r_high = cs.send(cx.at[3, high], rr.at[2, high], at_z(zr))
    cx[5, low, :] = own(5, low)
    l_low = cs.send(cx.at[5, low], rl.at[2, low], at_z(zl))
    r_low, l_high = far_r, far_l
    cx[3, low, :] = own(3, low)
    cx[5, high, :] = own(5, high)
    r_low.wait_recv()
    rr[3, low, :] = add(rr[3, low, :], cx[3, low, :])
    r_low = cs.send(rr.at[3, low], rr.at[2, low], at_z(zr))
    l_high.wait_recv()
    rl[3, high, :] = add(rl[3, high, :], cx[5, high, :])
    l_high = cs.send(rl.at[3, high], rl.at[2, high], at_z(zl))
    for s in (2, 1):
        swaps[s].wait_recv()
        swaps[8 - s].wait_recv()
        cx[s] = add(p_ref[((z + s) % 8) * 2 + c], cx[s])
        cx[8 - s] = add(p_ref[((z + 8 - s) % 8) * 2 + c], cx[8 - s])
        r_high.wait_recv()
        rr[s, high, :] = add(rr[s, high, :], cx[s, high, :])
        r_high = cs.send(rr.at[s, high], rr.at[s - 1, high], at_z(zr))
        l_low.wait_recv()
        rl[s, low, :] = add(rl[s, low, :], cx[8 - s, low, :])
        l_low = cs.send(rl.at[s, low], rl.at[s - 1, low], at_z(zl))
        r_low.wait_recv()
        rr[s, low, :] = add(rr[s, low, :], cx[s, low, :])
        r_low = cs.send(rr.at[s, low], rr.at[s - 1, low], at_z(zr))
        l_high.wait_recv()
        rl[s, high, :] = add(rl[s, high, :], cx[8 - s, high, :])
        l_high = cs.send(rl.at[s, high], rl.at[s - 1, high], at_z(zl))
    swaps[0].wait_recv()
    r_high.wait_recv()
    l_low.wait_recv()
    r_low.wait_recv()
    l_high.wait_recv()
    out_ref[...] = (
        p_ref[z * 2 + c].astype(jnp.float32)
        + cx[0].astype(jnp.float32)
        + rr[0].astype(jnp.float32)
        + rl[0].astype(jnp.float32)
    ).astype(jnp.bfloat16)
    cs.finish()


def scatter_sum(partial):
    blocks, t, width = partial.shape
    whole = pl.BlockSpec(memory_space=pltpu.VMEM)
    return pl.pallas_call(
        scatter_kernel,
        out_shape=jax.ShapeDtypeStruct((t, width), partial.dtype),
        in_specs=[whole],
        out_specs=whole,
        scratch_shapes=[
            pltpu.VMEM((8, t, width), jnp.bfloat16),
            pltpu.VMEM((4, t, width), jnp.bfloat16),
            pltpu.VMEM((4, t, width), jnp.bfloat16),
            pltpu.SemaphoreType.DMA((N_SCATTER,)),
            pltpu.SemaphoreType.DMA((N_SCATTER,)),
        ],
        compiler_params=pltpu.CompilerParams(
            collective_id=1, has_side_effects=True, vmem_limit_bytes=48 * 1024 * 1024
        ),
        cost_estimate=pl.CostEstimate(flops=0, bytes_accessed=200_000_000, transcendentals=0),
        name="scatter_sum",
    )(partial)


def adam_update(weight, gradient, first_moment, second_moment):
    first_next = BETA_ONE * first_moment.astype(jnp.float32) + (1.0 - BETA_ONE) * gradient
    second_next = (
        BETA_TWO * second_moment.astype(jnp.float32) + (1.0 - BETA_TWO) * gradient * gradient
    )
    stepped = weight.astype(jnp.float32) - LEARNING_RATE * (first_next * CORRECT_FIRST) / (
        jnp.sqrt(second_next * CORRECT_SECOND) + EPSILON
    )
    return (
        stepped.astype(jnp.bfloat16),
        first_next.astype(jnp.bfloat16),
        second_next.astype(jnp.bfloat16),
    )


def slot_ranks(flat_routes, expert_count):
    onehot = (flat_routes[:, None] == jnp.arange(expert_count, dtype=jnp.int32)[None, :]).astype(
        jnp.int32
    )
    ranks = jnp.cumsum(onehot, axis=0) - 1
    return jnp.sum(ranks * onehot, axis=1)


def in_three(values):
    high = values.astype(jnp.bfloat16)
    rest = values - high.astype(jnp.float32)
    middle = rest.astype(jnp.bfloat16)
    low = (rest - middle.astype(jnp.float32)).astype(jnp.bfloat16)
    return [high, middle, low]


def local(
    tokens,
    routes,
    combine_weight,
    owner_plan,
    w_in,
    w_out,
    grad_in,
    grad_out,
    first_in,
    second_in,
    first_out,
    second_out,
):
    token_count, route_count = routes.shape
    width = tokens.shape[1]
    half = width // 2
    expert_count = owner_plan.shape[0]
    dp = lax.axis_index("dp")
    flat_routes = routes.reshape(-1)
    ranks = slot_ranks(flat_routes, expert_count).reshape(token_count, route_count)
    packed = [routes.astype(jnp.bfloat16), ranks.astype(jnp.bfloat16)] + in_three(combine_weight)
    spare = jnp.zeros((token_count, EXTRA - 5 * route_count), jnp.bfloat16)
    tok = jnp.concatenate([tokens] + packed + [spare], 1)
    grads = jnp.concatenate([grad_in[0], grad_out], 0)
    mine = lax.dynamic_slice_in_dim(grads, dp * half, half, 2)
    other = lax.dynamic_slice_in_dim(grads, (1 - dp) * half, half, 2)
    came = lax.ppermute(other, "dp", [(0, 1), (1, 0)])
    summed = mine.astype(jnp.float32) + came.astype(jnp.float32)
    weights = jnp.concatenate([w_in, w_out[None]], 0)
    firsts = jnp.concatenate([first_in, first_out[None]], 0)
    seconds = jnp.concatenate([second_in, second_out[None]], 0)
    new_w, first_next, second_next = adam_update(weights, summed, firsts, seconds)
    groups = expert_count
    both = jnp.concatenate([first_next.reshape(-1, half), second_next.reshape(-1, half)], 0)
    chunk = both.shape[0] // groups
    spread = lax.all_to_all(
        both.reshape(groups, chunk, half), ("yl", "z", "xh"), 0, 0, tiled=True
    )
    picked = jnp.take(spread, owner_plan, axis=0)
    landed = lax.all_to_all(picked, ("yl", "z", "xh"), 0, 0, tiled=True).reshape(both.shape)
    landed = landed.reshape(2, 3, -1, half)
    all_tok, all_w = gather_all(tok, new_w)
    partial = experts(all_tok, all_w, width, route_count)
    combined = scatter_sum(partial)
    return (
        combined,
        landed[0, :2],
        landed[1, :2],
        landed[0, 2],
        landed[1, 2],
    )


def solution(mesh):
    devices = mesh.devices.reshape(2, 8, 2, 2, 2, 2)
    inner = Mesh(devices, EX + ("dp",))
    both = EX + ("dp",)
    in_specs = (
        P(both, None),
        P(both, None),
        P(both, None),
        P(),
        P(None, EX, "dp"),
        P(EX, "dp"),
        P("dp", None, EX, None),
        P("dp", EX, None),
        P(None, EX, "dp"),
        P(None, EX, "dp"),
        P(EX, "dp"),
        P(EX, "dp"),
    )
    out_specs = (
        P(both, None),
        P(None, EX, "dp"),
        P(None, EX, "dp"),
        P(EX, "dp"),
        P(EX, "dp"),
    )
    return jax.shard_map(local, mesh=inner, in_specs=in_specs, out_specs=out_specs, check_vma=False)
```
